32 devices in a mesh: clips: 2 (over x), tm: 4 (over y, core), height: 4 (over z).
Axes of the slice: x: 2, y: 2, z: 4, core: 2. Of those that a mesh axis runs over, the one named last changes fastest.
Arguments:
- features: bfloat16 [16, 16, 96, 512], P(('clips', 'tm'), 'height'), parts along dimension 0, may hold values from -1000 to 1000
- gain: float32 [512], replicated, may hold values from 0.1 to 1.9
- shift: float32 [512], replicated, may hold values from -3 to 3
- kernel: bfloat16 [3, 3, 3, 512, 256], replicated, may hold values from -0.0546875 to 0.0546875
- bias: float32 [256], replicated, may hold values from -3 to 3
Outputs:
- decoded: bfloat16 [16, 16, 96, 256], P(('clips', 'tm'), 'height'), parts along dimension 0
The draws below stay inside these ranges and needn't reach their ends.
There are 2 independent parts, one for each index of `clips`. The reference program is written for one: setup_inputs(seed, part) draws one part's arguments, and reference() takes and returns one part's arrays. A program takes and returns all parts, laid end to end along the dimension named above; an argument that names none is the same for every part. Nothing has to cross between parts.
All inputs are finite; a program needn't handle non-finite values.
Results may differ from the reference program's by a relative error of at most 0.0055.
Values may be sent and summed in bfloat16 or wider, within the bound.
A program may use at most 64 MiB of HBM per device.

```python
import jax
import jax.numpy as jnp
from jax import lax

CHANNELS = 512
COUT = 256
GROUPS = 32
COLS = 96
FRAMES = 8
ROWS = 16


def draw_features(key, part):
    keys = jax.random.split(jax.random.fold_in(key, 17), 5)
    frame_pos = jnp.arange(FRAMES, dtype=jnp.float32) / max(FRAMES - 1, 1)
    frame_trend = jnp.exp(jnp.log(3.0) * frame_pos)
    chan_scale = jnp.exp(jax.random.uniform(keys[1], (CHANNELS,), jnp.float32, 0.0, jnp.log(10.0)))
    chan_offset = 0.5 * jax.random.normal(keys[2], (CHANNELS,), jnp.float32)
    noise = jnp.clip(jax.random.normal(keys[0], (FRAMES, ROWS, COLS, CHANNELS), jnp.float32), -6.0, 6.0)
    frame_random = jnp.exp(jax.random.uniform(keys[4], (FRAMES,), jnp.float32, -jnp.log(2.0), jnp.log(2.0)))
    frame_scale = frame_trend * frame_random
    values = (noise + chan_offset) * chan_scale
    values = values * frame_scale[:, None, None, None]
    values = jnp.clip(values, -1000.0, 1000.0)
    return values.astype(jnp.bfloat16)


def bell_draw(stream_key, extent, deviation, reach, held_as=jnp.bfloat16):
    result = deviation * jax.random.normal(stream_key, extent, jnp.float32)
    return jnp.clip(result, min=-reach, max=reach).astype(held_as)


def setup_inputs(seed: int = 0, part: int = 0) -> dict:
    key_list = jax.random.split(jax.random.key(seed), 6)
    part_splits = jax.random.split(jax.random.fold_in(key_list[5], part), 6)
    features = draw_features(jax.random.fold_in(jax.random.fold_in(key_list[5], part), 71), part)
    gain = jnp.clip(1.0 + 0.18 * jax.random.normal(key_list[1], (CHANNELS,), jnp.float32), 0.1, 1.9)
    shift = bell_draw(key_list[2], (CHANNELS,), 0.5, 3.0, jnp.float32)
    kernel = bell_draw(key_list[3], (3, 3, 3, CHANNELS, COUT), (27 * CHANNELS) ** -0.5, 0.0546875)
    bias = bell_draw(key_list[4], (COUT,), 0.5, 3.0, jnp.float32)
    return {"features": features, "gain": gain, "shift": shift, "kernel": kernel, "bias": bias}


epsilon = 1e-06

def reference(features, gain, shift, kernel, bias):
    per_group = CHANNELS // GROUPS
    wide_values = features.astype(jnp.float32).reshape(FRAMES, ROWS, COLS, GROUPS, per_group)
    cells_total = FRAMES * ROWS * COLS * per_group
    group_mean = lax.optimization_barrier(jnp.sum(wide_values, axis=(0, 1, 2, 4))) / cells_total
    centered = wide_values - group_mean[:, None]
    group_var = lax.optimization_barrier(jnp.sum(centered * centered, axis=(0, 1, 2, 4))) / cells_total
    normed = centered * lax.rsqrt(group_var + epsilon)[:, None]
    normed = normed.reshape(FRAMES, ROWS, COLS, CHANNELS) * gain + shift
    activated = jax.nn.silu(normed).astype(jnp.bfloat16)
    padded = jnp.concatenate([activated[:1], activated[:1], activated], 0)
    padded = jnp.pad(padded, ((0, 0), (1, 1), (1, 1), (0, 0)))

    def one_frame(position):
        slab = lax.dynamic_slice_in_dim(padded, position, 3, 0)
        summed = jnp.zeros((ROWS * COLS, COUT), jnp.float32)
        for a in range(3):
            for b in range(3):
                for c in range(3):
                    window = slab[a, b:b + ROWS, c:c + COLS, :].reshape(ROWS * COLS, CHANNELS)
                    summed = summed + jnp.dot(window, kernel[a, b, c], preferred_element_type=jnp.float32)
        return (summed.reshape(ROWS, COLS, COUT) + bias).astype(jnp.bfloat16)
    return lax.map(one_frame, jnp.arange(FRAMES, dtype=jnp.int32))
```

```python
import functools

import jax
import jax.numpy as jnp
from jax import lax
from jax.experimental import pallas as pl
from jax.experimental.pallas import tpu as pltpu
from jax.sharding import PartitionSpec as P

GROUPS = 32
EPSILON = 1e-06
MESH = pl.DeviceIdType.MESH
F32 = jnp.float32
BF16 = jnp.bfloat16


def group_sums(values, per_group):
    lanes = values.shape[-1]
    lane = lax.broadcasted_iota(jnp.int32, values.shape, values.ndim - 1)
    step = 1
    while step < per_group:
        up = pltpu.roll(values, lanes - step, values.ndim - 1)
        down = pltpu.roll(values, step, values.ndim - 1)
        values = values + jnp.where((lane & step) == 0, up, down)
        step *= 2
    return values


def body(
    n_tm,
    n_h,
    x_hbm,
    gain_ref,
    shift_ref,
    w_hbm,
    bias_ref,
    out_ref,
    x_vm,
    w_vm,
    top_vm,
    bot_vm,
    st1,
    st2,
    lhs,
    prod,
    nbuf,
    rbuf,
    x_sem,
    w_sem,
    s1_send,
    s1_recv,
    s2_send,
    s2_recv,
    h_send,
    h_recv,
    n_send,
    n_recv,
):
    frames, rows, cols, channels = x_vm.shape
    per_group = channels // GROUPS
    tm = lax.axis_index("tm")
    hh = lax.axis_index("height")

    barrier = pltpu.get_barrier_semaphore()
    for d in range(1, n_h):
        pl.semaphore_signal(
            barrier, inc=1, device_id={"height": lax.rem(hh + d, n_h)}, device_id_type=MESH
        )
    for d in range(1, n_tm):
        pl.semaphore_signal(
            barrier, inc=1, device_id={"tm": lax.rem(tm + d, n_tm)}, device_id_type=MESH
        )
    x_copy = pltpu.make_async_copy(x_hbm, x_vm, x_sem)
    x_copy.start()
    w_copies = [
        [pltpu.make_async_copy(w_hbm.at[a, :, c], w_vm.at[a, c], w_sem.at[a, c]) for c in range(3)]
        for a in range(3)
    ]
    for a in range(3):
        for c in range(3):
            w_copies[a][c].start()

    x_copy.wait()
    sums = jnp.zeros((8, channels), F32)
    squares = jnp.zeros((8, channels), F32)
    for f in range(frames):
        for r in range(rows):
            v = x_vm[f, r].astype(F32).reshape(cols // 8, 8, channels)
            sums = sums + jnp.sum(v, axis=0)
            squares = squares + jnp.sum(v * v, axis=0)
    st1[0, 0:1] = jnp.sum(sums, axis=0, keepdims=True)
    st1[0, 1:2] = jnp.sum(squares, axis=0, keepdims=True)

    pl.semaphore_wait(barrier, n_h + n_tm - 2)

    def stage(buf, send, recv, axis, me, count):
        copies = []
        for d in range(1, count):
            copies.append(
                pltpu.make_async_remote_copy(
                    src_ref=buf.at[0],
                    dst_ref=buf.at[d],
                    send_sem=send.at[d],
                    recv_sem=recv.at[d],
                    device_id={axis: lax.rem(me + d, count)},
                    device_id_type=MESH,
                )
            )
        return copies

    stage1 = stage(st1, s1_send, s1_recv, "tm", tm, n_tm)
    stage2 = stage(st2, s2_send, s2_recv, "height", hh, n_h)
    for copy in stage1:
        copy.start()
    to_next = pltpu.make_async_remote_copy(
        src_ref=x_hbm.at[:, rows - 1],
        dst_ref=top_vm,
        send_sem=h_send.at[0],
        recv_sem=h_recv.at[0],
        device_id={"height": lax.rem(hh + 1, n_h)},
        device_id_type=MESH,
    )
    to_last = pltpu.make_async_remote_copy(
        src_ref=x_hbm.at[:, 0],
        dst_ref=bot_vm,
        send_sem=h_send.at[1],
        recv_sem=h_recv.at[1],
        device_id={"height": lax.rem(hh + n_h - 1, n_h)},
        device_id_type=MESH,
    )
    total = st1[0]
    for d in range(1, n_tm):
        stage1[d - 1].wait_recv()
        total = total + st1[d]
    st2[0] = total
    for copy in stage2:
        copy.start()

    @pl.when(hh < n_h - 1)
    def _():
        to_next.start()

    @pl.when(hh > 0)
    def _():
        to_last.start()

    for d in range(1, n_h):
        stage2[d - 1].wait_recv()
        total = total + st2[d]
    cells = n_tm * n_h * frames * rows * cols * per_group
    means = group_sums(total, per_group) / cells
    mean = means[0:1]
    var = jnp.maximum(means[1:2] - mean * mean, 0.0)
    scale = gain_ref[...] * lax.rsqrt(var + EPSILON)
    half_offset = 0.5 * (shift_ref[...] - mean * scale)
    half_scale = 0.5 * scale

    def activate(v):
        h = v.astype(F32) * half_scale + half_offset
        return (h + h * jnp.tanh(h)).astype(BF16)

    row_sets = (tuple(range(1, rows - 1)), (0, rows - 1))
    per_set = 2 * cols

    def place(row, f, value):
        for s in range(2):
            for q, i in enumerate(row_sets[s]):
                b = row - i + 1
                if 0 <= b <= 2:
                    lhs[
                        s,
                        f * per_set + q * cols : f * per_set + (q + 1) * cols,
                        b * channels : (b + 1) * channels,
                    ] = value

    for f in range(frames):
        for r in range(rows):
            place(r, f, activate(x_vm[f, r]))

    m = frames * per_set
    position = lax.rem(lax.broadcasted_iota(jnp.int32, (m, 1), 0), cols)
    not_first = position != 0
    not_last = position != cols - 1

    def product(a, s):
        def tap(c):
            weights = w_vm[a, c].reshape(3 * channels, w_vm.shape[-1])
            return jnp.dot(lhs[s], weights, preferred_element_type=F32)

        low = jnp.where(not_first, pltpu.roll(tap(0), 1, 0), 0.0)
        high = jnp.where(not_last, pltpu.roll(tap(2), m - 1, 0), 0.0)
        prod[a, s] = low + tap(1) + high

    def sends(s, k):
        return pltpu.make_async_remote_copy(
            src_ref=nbuf.at[s, k],
            dst_ref=rbuf.at[s, k],
            send_sem=n_send.at[s, k],
            recv_sem=n_recv.at[s, k],
            device_id={"tm": lax.rem(tm + 1, n_tm)},
            device_id_type=MESH,
        )

    def send(s, k):
        @pl.when(tm < n_tm - 1)
        def _():
            sends(s, k).start()

    def wait_weights(a):
        for c in range(3):
            w_copies[a][c].wait()

    def early(s):
        if s == 0:
            wait_weights(0)
        product(0, s)
        nbuf[s, 1] = prod[0, s, per_set:].astype(BF16)
        send(s, 1)
        if s == 0:
            wait_weights(1)
        product(1, s)
        nbuf[s, 0] = (prod[0, s, :per_set] + prod[1, s, per_set:]).astype(BF16)
        send(s, 0)

        @pl.when(tm == 0)
        def _():
            rbuf[s, 0] = (prod[0, s, :per_set] + prod[1, s, :per_set]).astype(BF16)
            rbuf[s, 1] = prod[0, s, :per_set].astype(BF16)

    early(0)

    @pl.when(hh > 0)
    def _():
        to_next.wait_recv()
        for f in range(frames):
            place(-1, f, activate(top_vm[f]))

    @pl.when(hh == 0)
    def _():
        for f in range(frames):
            place(-1, f, jnp.zeros((cols, channels), BF16))

    @pl.when(hh < n_h - 1)
    def _():
        to_last.wait_recv()
        for f in range(frames):
            place(rows, f, activate(bot_vm[f]))

    @pl.when(hh == n_h - 1)
    def _():
        for f in range(frames):
            place(rows, f, jnp.zeros((cols, channels), BF16))

    early(1)
    wait_weights(2)
    product(2, 0)
    product(2, 1)

    bias = bias_ref[...]
    for s in range(2):
        for k in (1, 0):

            @pl.when(tm > 0)
            def _():
                sends(s, k).wait_recv()

            own = prod[2, s, k * per_set : (k + 1) * per_set]
            if k == 1:
                own = own + prod[1, s, :per_set]
            value = (own + rbuf[s, k].astype(F32) + bias).astype(BF16)
            for q, i in enumerate(row_sets[s]):
                out_ref[k, i] = value[q * cols : (q + 1) * cols]

    for copy in stage1 + stage2:
        copy.wait_send()

    @pl.when(hh < n_h - 1)
    def _():
        to_next.wait_send()

    @pl.when(hh > 0)
    def _():
        to_last.wait_send()

    @pl.when(tm < n_tm - 1)
    def _():
        for s in range(2):
            for k in range(2):
                sends(s, k).wait_send()


def solution(mesh):
    n_tm, n_h = mesh.shape["tm"], mesh.shape["height"]

    def on_device(features, gain, shift, kernel, bias):
        frames, rows, cols, channels = features.shape
        c_out = kernel.shape[-1]
        assert frames == 2 and rows == 4
        per_set = 2 * cols
        vmem = pl.BlockSpec(memory_space=pltpu.VMEM)
        anywhere = pl.BlockSpec(memory_space=pl.ANY)
        dma = pltpu.SemaphoreType.DMA
        return pl.pallas_call(
            functools.partial(body, n_tm, n_h),
            out_shape=jax.ShapeDtypeStruct((frames, rows, cols, c_out), BF16),
            in_specs=[anywhere, vmem, vmem, anywhere, vmem],
            out_specs=vmem,
            scratch_shapes=[
                pltpu.VMEM((frames, rows, cols, channels), BF16),
                pltpu.VMEM((3, 3, 3, channels, c_out), BF16),
                pltpu.VMEM((frames, cols, channels), BF16),
                pltpu.VMEM((frames, cols, channels), BF16),
                pltpu.VMEM((n_tm, 2, channels), F32),
                pltpu.VMEM((n_h, 2, channels), F32),
                pltpu.VMEM((2, frames * per_set, 3 * channels), BF16),
                pltpu.VMEM((3, 2, frames * per_set, c_out), F32),
                pltpu.VMEM((2, 2, per_set, c_out), BF16),
                pltpu.VMEM((2, 2, per_set, c_out), BF16),
                dma,
                dma((3, 3)),
                dma((n_tm,)),
                dma((n_tm,)),
                dma((n_h,)),
                dma((n_h,)),
                dma((2,)),
                dma((2,)),
                dma((2, 2)),
                dma((2, 2)),
            ],
            compiler_params=pltpu.CompilerParams(collective_id=0, has_side_effects=True),
        )(features, gain.reshape(1, -1), shift.reshape(1, -1), kernel, bias.reshape(1, -1))

    placed = (P(("clips", "tm"), "height", None, None), P(), P(), P(), P())
    return jax.shard_map(
        on_device,
        mesh=mesh,
        in_specs=placed,
        out_specs=P(("clips", "tm"), "height", None, None),
        check_vma=False,
    )
```

```python
import functools

import jax
import jax.numpy as jnp
from jax import lax
from jax.experimental import pallas as pl
from jax.experimental.pallas import tpu as pltpu
from jax.sharding import PartitionSpec as P

GROUPS = 32
EPSILON = 1e-06
MESH = pl.DeviceIdType.MESH
F32 = jnp.float32
BF16 = jnp.bfloat16


def group_sums(values, per_group):
    lanes = values.shape[-1]
    lane = lax.broadcasted_iota(jnp.int32, values.shape, values.ndim - 1)
    step = 1
    while step < per_group:
        up = pltpu.roll(values, lanes - step, values.ndim - 1)
        down = pltpu.roll(values, step, values.ndim - 1)
        values = values + jnp.where((lane & step) == 0, up, down)
        step *= 2
    return values


def body(
    n_tm,
    n_h,
    x_hbm,
    gain_hbm,
    shift_hbm,
    w_hbm,
    bias_hbm,
    out_ref,
    x_vm,
    gain_ref,
    shift_ref,
    bias_ref,
    w_vm,
    top_vm,
    bot_vm,
    stats,
    lhs,
    prod,
    nbuf,
    rbuf,
    x_sem,
    p_sem,
    w_sem,
    s_send,
    s_recv,
    h_send,
    h_recv,
    n_send,
    n_recv,
):
    frames, rows, cols, channels = x_vm.shape
    per_group = channels // GROUPS
    tm = lax.axis_index("tm")
    hh = lax.axis_index("height")

    barrier = pltpu.get_barrier_semaphore()
    count = n_tm * n_h
    me = tm * n_h + hh

    def peer(d):
        other = lax.rem(me + d, count)
        return {"tm": lax.div(other, n_h), "height": lax.rem(other, n_h)}

    for d in range(1, count):
        pl.semaphore_signal(barrier, inc=1, device_id=peer(d), device_id_type=MESH)
    x_copy = pltpu.make_async_copy(x_hbm, x_vm, x_sem)
    x_copy.start()
    small = ((gain_hbm, gain_ref), (shift_hbm, shift_ref), (bias_hbm, bias_ref))
    p_copies = [pltpu.make_async_copy(*pair, p_sem.at[i]) for i, pair in enumerate(small)]
    for copy in p_copies:
        copy.start()
    w_copies = [
        [pltpu.make_async_copy(w_hbm.at[a, :, c], w_vm.at[a, c], w_sem.at[a, c]) for c in range(3)]
        for a in range(3)
    ]
    x_copy.wait()
    for a in range(3):
        for c in range(3):
            w_copies[a][c].start()
    sums = jnp.zeros((8, channels), F32)
    squares = jnp.zeros((8, channels), F32)
    for f in range(frames):
        for r in range(rows):
            v = x_vm[f, r].astype(F32).reshape(cols // 8, 8, channels)
            sums = sums + jnp.sum(v, axis=0)
            squares = squares + jnp.sum(v * v, axis=0)
    stats[0, 0:1] = jnp.sum(sums, axis=0, keepdims=True)
    stats[0, 1:2] = jnp.sum(squares, axis=0, keepdims=True)

    pl.semaphore_wait(barrier, count - 1)

    shares = [
        pltpu.make_async_remote_copy(
            src_ref=stats.at[0],
            dst_ref=stats.at[d],
            send_sem=s_send.at[d],
            recv_sem=s_recv.at[d],
            device_id=peer(d),
            device_id_type=MESH,
        )
        for d in range(1, count)
    ]
    for copy in shares:
        copy.start()
    to_next = pltpu.make_async_remote_copy(
        src_ref=x_hbm.at[:, rows - 1],
        dst_ref=top_vm,
        send_sem=h_send.at[0],
        recv_sem=h_recv.at[0],
        device_id={"height": lax.rem(hh + 1, n_h)},
        device_id_type=MESH,
    )
    to_last = pltpu.make_async_remote_copy(
        src_ref=x_hbm.at[:, 0],
        dst_ref=bot_vm,
        send_sem=h_send.at[1],
        recv_sem=h_recv.at[1],
        device_id={"height": lax.rem(hh + n_h - 1, n_h)},
        device_id_type=MESH,
    )
    @pl.when(hh < n_h - 1)
    def _():
        to_next.start()

    @pl.when(hh > 0)
    def _():
        to_last.start()

    for copy in shares:
        copy.wait_recv()
    total = jnp.sum(stats[...], axis=0)
    for copy in p_copies:
        copy.wait()
    cells = n_tm * n_h * frames * rows * cols * per_group
    means = group_sums(total, per_group) / cells
    mean = means[0:1]
    var = jnp.maximum(means[1:2] - mean * mean, 0.0)
    scale = gain_ref[...] * lax.rsqrt(var + EPSILON)
    half_offset = 0.5 * (shift_ref[...] - mean * scale)
    half_scale = 0.5 * scale

    def activate(v):
        h = v.astype(F32) * half_scale + half_offset
        return (h + h * jnp.tanh(h)).astype(BF16)

    row_sets = (tuple(range(1, rows - 1)), (0, rows - 1))
    per_set = 2 * cols

    def place(row, f, value):
        for s in range(2):
            for q, i in enumerate(row_sets[s]):
                b = row - i + 1
                if 0 <= b <= 2:
                    lhs[
                        s,
                        f * per_set + q * cols : f * per_set + (q + 1) * cols,
                        b * channels : (b + 1) * channels,
                    ] = value

    for f in range(frames):
        for r in range(rows):
            place(r, f, activate(x_vm[f, r]))

    m = frames * per_set
    position = lax.rem(lax.broadcasted_iota(jnp.int32, (m, 1), 0), cols)
    not_first = position != 0
    not_last = position != cols - 1

    def product(a, s):
        def tap(c):
            weights = w_vm[a, c].reshape(3 * channels, w_vm.shape[-1])
            return jnp.dot(lhs[s], weights, preferred_element_type=F32)

        low = jnp.where(not_first, pltpu.roll(tap(0), 1, 0), 0.0)
        high = jnp.where(not_last, pltpu.roll(tap(2), m - 1, 0), 0.0)
        prod[a, s] = low + tap(1) + high

    def sends(s, k):
        return pltpu.make_async_remote_copy(
            src_ref=nbuf.at[s, k],
            dst_ref=rbuf.at[s, k],
            send_sem=n_send.at[s, k],
            recv_sem=n_recv.at[s, k],
            device_id={"tm": lax.rem(tm + 1, n_tm)},
            device_id_type=MESH,
        )

    def wait_weights(a):
        for c in range(3):
            w_copies[a][c].wait()

    def early(s):
        if s == 0:
            wait_weights(0)
            wait_weights(1)
        product(0, s)
        product(1, s)
        nbuf[s, 1] = prod[0, s, per_set:].astype(BF16)
        nbuf[s, 0] = (prod[0, s, :per_set] + prod[1, s, per_set:]).astype(BF16)

        @pl.when(tm < n_tm - 1)
        def _():
            sends(s, 1).start()
            sends(s, 0).start()

        @pl.when(tm == 0)
        def _():
            rbuf[s, 0] = (prod[0, s, :per_set] + prod[1, s, :per_set]).astype(BF16)
            rbuf[s, 1] = prod[0, s, :per_set].astype(BF16)

    early(0)

    @pl.when(hh > 0)
    def _():
        to_next.wait_recv()
        for f in range(frames):
            place(-1, f, activate(top_vm[f]))

    @pl.when(hh == 0)
    def _():
        for f in range(frames):
            place(-1, f, jnp.zeros((cols, channels), BF16))

    @pl.when(hh < n_h - 1)
    def _():
        to_last.wait_recv()
        for f in range(frames):
            place(rows, f, activate(bot_vm[f]))

    @pl.when(hh == n_h - 1)
    def _():
        for f in range(frames):
            place(rows, f, jnp.zeros((cols, channels), BF16))

    early(1)
    wait_weights(2)
    product(2, 0)
    product(2, 1)

    bias = bias_ref[...]
    for s in range(2):
        for k in (1, 0):

            @pl.when(tm > 0)
            def _():
                sends(s, k).wait_recv()

            own = prod[2, s, k * per_set : (k + 1) * per_set]
            if k == 1:
                own = own + prod[1, s, :per_set]
            value = (own + rbuf[s, k].astype(F32) + bias).astype(BF16)
            for q, i in enumerate(row_sets[s]):
                out_ref[k, i] = value[q * cols : (q + 1) * cols]

    for copy in shares:
        copy.wait_send()

    @pl.when(hh < n_h - 1)
    def _():
        to_next.wait_send()

    @pl.when(hh > 0)
    def _():
        to_last.wait_send()

    @pl.when(tm < n_tm - 1)
    def _():
        for s in range(2):
            for k in range(2):
                sends(s, k).wait_send()


def solution(mesh):
    n_tm, n_h = mesh.shape["tm"], mesh.shape["height"]

    def on_device(features, gain, shift, kernel, bias):
        frames, rows, cols, channels = features.shape
        c_out = kernel.shape[-1]
        assert frames == 2 and rows == 4
        per_set = 2 * cols
        vmem = pl.BlockSpec(memory_space=pltpu.VMEM)
        hbm = pl.BlockSpec(memory_space=pltpu.HBM)
        dma = pltpu.SemaphoreType.DMA
        return pl.pallas_call(
            functools.partial(body, n_tm, n_h),
            out_shape=pltpu.VMEM((frames, rows, cols, c_out), BF16),
            in_specs=[hbm] * 5,
            out_specs=vmem,
            scratch_shapes=[
                pltpu.VMEM((frames, rows, cols, channels), BF16),
                pltpu.VMEM((1, channels), F32),
                pltpu.VMEM((1, channels), F32),
                pltpu.VMEM((1, c_out), F32),
                pltpu.VMEM((3, 3, 3, channels, c_out), BF16),
                pltpu.VMEM((frames, cols, channels), BF16),
                pltpu.VMEM((frames, cols, channels), BF16),
                pltpu.VMEM((n_tm * n_h, 2, channels), F32),
                pltpu.VMEM((2, frames * per_set, 3 * channels), BF16),
                pltpu.VMEM((3, 2, frames * per_set, c_out), F32),
                pltpu.VMEM((2, 2, per_set, c_out), BF16),
                pltpu.VMEM((2, 2, per_set, c_out), BF16),
                dma,
                dma((3,)),
                dma((3, 3)),
                dma((n_tm * n_h,)),
                dma((n_tm * n_h,)),
                dma((2,)),
                dma((2,)),
                dma((2, 2)),
                dma((2, 2)),
            ],
            compiler_params=pltpu.CompilerParams(
                collective_id=0, has_side_effects=True, vmem_limit_bytes=67_043_328 - 640 * 2**10
            ),
        )(features, gain.reshape(1, -1), shift.reshape(1, -1), kernel, bias.reshape(1, -1))

    placed = (P(("clips", "tm"), "height", None, None), P(), P(), P(), P())
    return jax.shard_map(
        on_device,
        mesh=mesh,
        in_specs=placed,
        out_specs=P(("clips", "tm"), "height", None, None),
        check_vma=False,
    )
```

```python
import functools

import jax
import jax.numpy as jnp
from jax import lax
from jax.experimental import pallas as pl
from jax.experimental.pallas import tpu as pltpu
from jax.sharding import PartitionSpec as P

GROUPS = 32
EPSILON = 1e-06
MESH = pl.DeviceIdType.MESH
F32 = jnp.float32
BF16 = jnp.bfloat16


LANES = 128


def group_sums(values, group):
    lanes = values.shape[-1]
    lane = lax.broadcasted_iota(jnp.int32, values.shape, values.ndim - 1)
    step = 1
    while step < group:
        up = pltpu.roll(values, lanes - step, values.ndim - 1)
        down = pltpu.roll(values, step, values.ndim - 1)
        values = values + jnp.where((lane & step) == 0, up, down)
        step *= 2
    return values


def own_lanes(parts):
    lane = lax.broadcasted_iota(jnp.int32, (parts, LANES), 1)
    row = lax.broadcasted_iota(jnp.int32, (parts, LANES), 0)
    return lax.rem(lane, parts) == row


def body(
    n_tm,
    n_h,
    x_hbm,
    gain_hbm,
    shift_hbm,
    w_hbm,
    bias_hbm,
    out_ref,
    x_vm,
    gain_ref,
    shift_ref,
    bias_ref,
    w_vm,
    top_vm,
    bot_vm,
    stats,
    lhs,
    prod,
    nbuf,
    rbuf,
    x_sem,
    p_sem,
    w_sem,
    s_send,
    s_recv,
    h_send,
    h_recv,
    n_send,
    n_recv,
):
    frames, rows, cols, channels = x_vm.shape
    per_group = channels // GROUPS
    tm = lax.axis_index("tm")
    hh = lax.axis_index("height")

    barrier = pltpu.get_barrier_semaphore()
    count = n_tm * n_h
    me = tm * n_h + hh

    def peer(d):
        other = lax.rem(me + d, count)
        return {"tm": lax.div(other, n_h), "height": lax.rem(other, n_h)}

    for d in range(1, count):
        pl.semaphore_signal(barrier, inc=1, device_id=peer(d), device_id_type=MESH)
    x_copy = pltpu.make_async_copy(x_hbm, x_vm, x_sem)
    x_copy.start()
    small = ((gain_hbm, gain_ref), (shift_hbm, shift_ref), (bias_hbm, bias_ref))
    p_copies = [pltpu.make_async_copy(*pair, p_sem.at[i]) for i, pair in enumerate(small)]
    for copy in p_copies:
        copy.start()
    w_copies = [
        [pltpu.make_async_copy(w_hbm.at[a, :, c], w_vm.at[a, c], w_sem.at[a, c]) for c in range(3)]
        for a in range(3)
    ]
    x_copy.wait()
    for a in range(3):
        for c in range(3):
            w_copies[a][c].start()
    sums = jnp.zeros((8, channels), F32)
    squares = jnp.zeros((8, channels), F32)
    for f in range(frames):
        for r in range(rows):
            v = x_vm[f, r].astype(F32).reshape(cols // 8, 8, channels)
            sums = sums + jnp.sum(v, axis=0)
            squares = squares + jnp.sum(v * v, axis=0)
    blocks = channels // LANES
    parts = 2 * blocks
    assert parts <= per_group <= LANES
    sums = jnp.sum(sums, axis=0, keepdims=True)
    squares = jnp.sum(squares, axis=0, keepdims=True)
    stacked = jnp.concatenate(
        [v[:, k * LANES : (k + 1) * LANES] for v in (sums, squares) for k in range(blocks)], axis=0
    )
    spread = jnp.where(own_lanes(parts), group_sums(stacked, per_group), 0.0)
    stats[0] = jnp.sum(spread, axis=0, keepdims=True)

    pl.semaphore_wait(barrier, count - 1)

    shares = [
        pltpu.make_async_remote_copy(
            src_ref=stats.at[0],
            dst_ref=stats.at[d],
            send_sem=s_send.at[d],
            recv_sem=s_recv.at[d],
            device_id=peer(d),
            device_id_type=MESH,
        )
        for d in range(1, count)
    ]
    for copy in shares:
        copy.start()
    to_next = pltpu.make_async_remote_copy(
        src_ref=x_hbm.at[:, rows - 1],
        dst_ref=top_vm,
        send_sem=h_send.at[0],
        recv_sem=h_recv.at[0],
        device_id={"height": lax.rem(hh + 1, n_h)},
        device_id_type=MESH,
    )
    to_last = pltpu.make_async_remote_copy(
        src_ref=x_hbm.at[:, 0],
        dst_ref=bot_vm,
        send_sem=h_send.at[1],
        recv_sem=h_recv.at[1],
        device_id={"height": lax.rem(hh + n_h - 1, n_h)},
        device_id_type=MESH,
    )
    @pl.when(hh < n_h - 1)
    def _():
        to_next.start()

    @pl.when(hh > 0)
    def _():
        to_last.start()

    for copy in shares:
        copy.wait_recv()
    total = jnp.sum(stats[...], axis=0)
    for copy in p_copies:
        copy.wait()
    cells = n_tm * n_h * frames * rows * cols * per_group
    means = group_sums(jnp.where(own_lanes(parts), total, 0.0), parts) * (1.0 / cells)
    mean = means[:blocks]
    var = jnp.maximum(means[blocks:] - mean * mean, 0.0)
    inverse = lax.rsqrt(var + EPSILON)

    def one_row(v):
        return jnp.concatenate([v[k : k + 1] for k in range(blocks)], axis=1)

    half_scale = 0.5 * gain_ref[...] * one_row(inverse)
    half_offset = 0.5 * shift_ref[...] - one_row(mean) * half_scale

    def activate(v):
        h = v.astype(F32) * half_scale + half_offset
        return (h + h * jnp.tanh(h)).astype(BF16)

    row_sets = (tuple(range(1, rows - 1)), (0, rows - 1))
    per_set = 2 * cols

    def place(row, f, value):
        for s in range(2):
            for q, i in enumerate(row_sets[s]):
                b = row - i + 1
                if 0 <= b <= 2:
                    lhs[
                        s,
                        f * per_set + q * cols : f * per_set + (q + 1) * cols,
                        b * channels : (b + 1) * channels,
                    ] = value

    for f in range(frames):
        for r in range(rows):
            place(r, f, activate(x_vm[f, r]))

    m = frames * per_set
    position = lax.rem(lax.broadcasted_iota(jnp.int32, (m, 1), 0), cols)
    not_first = position != 0
    not_last = position != cols - 1

    def product(a, s):
        def tap(c, start, stop):
            weights = w_vm[a, c].reshape(3 * channels, w_vm.shape[-1])
            return jnp.dot(lhs[s, start:stop], weights, preferred_element_type=F32)

        low = jnp.where(not_first, pltpu.roll(tap(0, 0, m), 1, 0), 0.0)
        high = jnp.where(not_last, pltpu.roll(tap(2, 0, m), m - 1, 0), 0.0)
        sides = low + high
        for start in (0, per_set):
            stop = start + per_set
            prod[a, s, start:stop] = sides[start:stop] + tap(1, start, stop)

    def sends(s, k):
        return pltpu.make_async_remote_copy(
            src_ref=nbuf.at[s, k],
            dst_ref=rbuf.at[s, k],
            send_sem=n_send.at[s, k],
            recv_sem=n_recv.at[s, k],
            device_id={"tm": lax.rem(tm + 1, n_tm)},
            device_id_type=MESH,
        )

    def send(s, k):
        @pl.when(tm < n_tm - 1)
        def _():
            sends(s, k).start()

    def wait_weights(a):
        for c in range(3):
            w_copies[a][c].wait()

    def early(s):
        if s == 0:
            wait_weights(0)
            wait_weights(1)
        product(0, s)
        nbuf[s, 1] = prod[0, s, per_set:].astype(BF16)
        send(s, 1)
        product(1, s)
        nbuf[s, 0] = (prod[0, s, :per_set] + prod[1, s, per_set:]).astype(BF16)
        send(s, 0)

    early(0)

    @pl.when(hh > 0)
    def _():
        to_next.wait_recv()
        for f in range(frames):
            place(-1, f, activate(top_vm[f]))

    @pl.when(hh == 0)
    def _():
        for f in range(frames):
            place(-1, f, jnp.zeros((cols, channels), BF16))

    @pl.when(hh < n_h - 1)
    def _():
        to_last.wait_recv()
        for f in range(frames):
            place(rows, f, activate(bot_vm[f]))

    @pl.when(hh == n_h - 1)
    def _():
        for f in range(frames):
            place(rows, f, jnp.zeros((cols, channels), BF16))

    wait_weights(2)
    early(1)
    product(2, 0)
    product(2, 1)

    bias = bias_ref[...]
    for s in range(2):
        for k in (1, 0):

            @pl.when(tm > 0)
            def _():
                sends(s, k).wait_recv()

            own = prod[2, s, k * per_set : (k + 1) * per_set]
            first = prod[0, s, :per_set]
            other = prod[1, s, :per_set]
            if k == 1:
                own = own + other
            else:
                first = first + other
            earlier = jnp.where(tm == 0, first, rbuf[s, k].astype(F32))
            value = (own + earlier + bias).astype(BF16)
            for q, i in enumerate(row_sets[s]):
                out_ref[k, i] = value[q * cols : (q + 1) * cols]

    for copy in shares:
        copy.wait_send()

    @pl.when(hh < n_h - 1)
    def _():
        to_next.wait_send()

    @pl.when(hh > 0)
    def _():
        to_last.wait_send()

    @pl.when(tm < n_tm - 1)
    def _():
        for s in range(2):
            for k in range(2):
                sends(s, k).wait_send()


def solution(mesh):
    n_tm, n_h = mesh.shape["tm"], mesh.shape["height"]

    def on_device(features, gain, shift, kernel, bias):
        frames, rows, cols, channels = features.shape
        c_out = kernel.shape[-1]
        assert frames == 2 and rows == 4
        per_set = 2 * cols
        vmem = pl.BlockSpec(memory_space=pltpu.VMEM)
        hbm = pl.BlockSpec(memory_space=pltpu.HBM)
        dma = pltpu.SemaphoreType.DMA
        return pl.pallas_call(
            functools.partial(body, n_tm, n_h),
            out_shape=pltpu.VMEM((frames, rows, cols, c_out), BF16),
            in_specs=[hbm] * 5,
            out_specs=vmem,
            scratch_shapes=[
                pltpu.VMEM((frames, rows, cols, channels), BF16),
                pltpu.VMEM((1, channels), F32),
                pltpu.VMEM((1, channels), F32),
                pltpu.VMEM((1, c_out), F32),
                pltpu.VMEM((3, 3, 3, channels, c_out), BF16),
                pltpu.VMEM((frames, cols, channels), BF16),
                pltpu.VMEM((frames, cols, channels), BF16),
                pltpu.VMEM((n_tm * n_h, 1, LANES), F32),
                pltpu.VMEM((2, frames * per_set, 3 * channels), BF16),
                pltpu.VMEM((3, 2, frames * per_set, c_out), F32),
                pltpu.VMEM((2, 2, per_set, c_out), BF16),
                pltpu.VMEM((2, 2, per_set, c_out), BF16),
                dma,
                dma((3,)),
                dma((3, 3)),
                dma((n_tm * n_h,)),
                dma((n_tm * n_h,)),
                dma((2,)),
                dma((2,)),
                dma((2, 2)),
                dma((2, 2)),
            ],
            compiler_params=pltpu.CompilerParams(
                collective_id=0, has_side_effects=True, vmem_limit_bytes=67_043_328 - 640 * 2**10
            ),
        )(features, gain.reshape(1, -1), shift.reshape(1, -1), kernel, bias.reshape(1, -1))

    placed = (P(("clips", "tm"), "height", None, None), P(), P(), P(), P())
    return jax.shard_map(
        on_device,
        mesh=mesh,
        in_specs=placed,
        out_specs=P(("clips", "tm"), "height", None, None),
        check_vma=False,
    )
```

```python
import functools

import jax
import jax.numpy as jnp
from jax import lax
from jax.experimental import pallas as pl
from jax.experimental.pallas import tpu as pltpu
from jax.sharding import PartitionSpec as P

GROUPS = 32
EPSILON = 1e-06
MESH = pl.DeviceIdType.MESH
F32 = jnp.float32
BF16 = jnp.bfloat16


LANES = 128


def group_sums(values, group):
    lanes = values.shape[-1]
    lane = lax.broadcasted_iota(jnp.int32, values.shape, values.ndim - 1)
    step = 1
    while step < group:
        up = pltpu.roll(values, lanes - step, values.ndim - 1)
        down = pltpu.roll(values, step, values.ndim - 1)
        values = values + jnp.where((lane & step) == 0, up, down)
        step *= 2
    return values


def own_lanes(parts):
    lane = lax.broadcasted_iota(jnp.int32, (parts, LANES), 1)
    row = lax.broadcasted_iota(jnp.int32, (parts, LANES), 0)
    return lax.rem(lane, parts) == row


def body(
    n_tm,
    n_h,
    x_hbm,
    gain_hbm,
    shift_hbm,
    w_hbm,
    bias_hbm,
    out_ref,
    x_vm,
    gain_ref,
    shift_ref,
    bias_ref,
    w_vm,
    top_vm,
    bot_vm,
    stats,
    lhs,
    prod,
    nbuf,
    rbuf,
    x_sem,
    p_sem,
    w_sem,
    s_send,
    s_recv,
    h_send,
    h_recv,
    n_send,
    n_recv,
):
    frames, rows, cols, channels = x_vm.shape
    per_group = channels // GROUPS
    tm = lax.axis_index("tm")
    hh = lax.axis_index("height")

    barrier = pltpu.get_barrier_semaphore()
    count = n_tm * n_h
    me = tm * n_h + hh

    def peer(d):
        other = lax.rem(me + d, count)
        return {"tm": lax.div(other, n_h), "height": lax.rem(other, n_h)}

    for d in range(1, count):
        pl.semaphore_signal(barrier, inc=1, device_id=peer(d), device_id_type=MESH)
    x_copies = [pltpu.make_async_copy(x_hbm.at[f], x_vm.at[f], x_sem.at[f]) for f in range(frames)]
    for copy in x_copies:
        copy.start()
    small = ((gain_hbm, gain_ref), (shift_hbm, shift_ref), (bias_hbm, bias_ref))
    p_copies = [pltpu.make_async_copy(*pair, p_sem.at[i]) for i, pair in enumerate(small)]
    for copy in p_copies:
        copy.start()
    w_copies = [
        [pltpu.make_async_copy(w_hbm.at[a, :, c], w_vm.at[a, c], w_sem.at[a, c]) for c in range(3)]
        for a in range(3)
    ]
    sums = jnp.zeros((8, channels), F32)
    squares = jnp.zeros((8, channels), F32)
    for f in range(frames):
        x_copies[f].wait()
        for r in range(rows):
            v = x_vm[f, r].astype(F32).reshape(cols // 8, 8, channels)
            sums = sums + jnp.sum(v, axis=0)
            squares = squares + jnp.sum(v * v, axis=0)
    blocks = channels // LANES
    parts = 2 * blocks
    assert parts <= per_group <= LANES
    sums = jnp.sum(sums, axis=0, keepdims=True)
    squares = jnp.sum(squares, axis=0, keepdims=True)
    stacked = jnp.concatenate(
        [v[:, k * LANES : (k + 1) * LANES] for v in (sums, squares) for k in range(blocks)], axis=0
    )
    spread = jnp.where(own_lanes(parts), group_sums(stacked, per_group), 0.0)
    stats[0] = jnp.sum(spread, axis=0, keepdims=True)

    pl.semaphore_wait(barrier, count - 1)

    shares = [
        pltpu.make_async_remote_copy(
            src_ref=stats.at[0],
            dst_ref=stats.at[d],
            send_sem=s_send.at[d],
            recv_sem=s_recv.at[d],
            device_id=peer(d),
            device_id_type=MESH,
        )
        for d in range(1, count)
    ]
    for copy in shares:
        copy.start()
    for a in range(3):
        for c in range(3):
            w_copies[a][c].start()
    to_next = pltpu.make_async_remote_copy(
        src_ref=x_hbm.at[:, rows - 1],
        dst_ref=top_vm,
        send_sem=h_send.at[0],
        recv_sem=h_recv.at[0],
        device_id={"height": lax.rem(hh + 1, n_h)},
        device_id_type=MESH,
    )
    to_last = pltpu.make_async_remote_copy(
        src_ref=x_hbm.at[:, 0],
        dst_ref=bot_vm,
        send_sem=h_send.at[1],
        recv_sem=h_recv.at[1],
        device_id={"height": lax.rem(hh + n_h - 1, n_h)},
        device_id_type=MESH,
    )
    @pl.when(hh < n_h - 1)
    def _():
        to_next.start()

    @pl.when(hh > 0)
    def _():
        to_last.start()

    for copy in shares:
        copy.wait_recv()
    total = jnp.sum(stats[...], axis=0)
    for copy in p_copies:
        copy.wait()
    cells = n_tm * n_h * frames * rows * cols * per_group
    means = group_sums(jnp.where(own_lanes(parts), total, 0.0), parts) * (1.0 / cells)
    mean = means[:blocks]
    var = jnp.maximum(means[blocks:] - mean * mean, 0.0)
    inverse = lax.rsqrt(var + EPSILON)

    def one_row(v):
        return jnp.concatenate([v[k : k + 1] for k in range(blocks)], axis=1)

    half_scale = 0.5 * gain_ref[...] * one_row(inverse)
    half_offset = 0.5 * shift_ref[...] - one_row(mean) * half_scale

    def activate(v):
        h = v.astype(F32) * half_scale + half_offset
        return (h + h * jnp.tanh(h)).astype(BF16)

    row_sets = (tuple(range(1, rows - 1)), (0, rows - 1))
    per_set = 2 * cols

    def place(row, f, value):
        for s in range(2):
            for q, i in enumerate(row_sets[s]):
                b = row - i + 1
                if 0 <= b <= 2:
                    lhs[
                        s,
                        f * per_set + q * cols : f * per_set + (q + 1) * cols,
                        b * channels : (b + 1) * channels,
                    ] = value

    for f in range(frames):
        for r in range(rows):
            place(r, f, activate(x_vm[f, r]))

    m = frames * per_set
    position = lax.rem(lax.broadcasted_iota(jnp.int32, (m, 1), 0), cols)
    not_first = position != 0
    not_last = position != cols - 1

    def product(a, s):
        def tap(c, start, stop):
            weights = w_vm[a, c].reshape(3 * channels, w_vm.shape[-1])
            return jnp.dot(lhs[s, start:stop], weights, preferred_element_type=F32)

        low = jnp.where(not_first, pltpu.roll(tap(0, 0, m), 1, 0), 0.0)
        high = jnp.where(not_last, pltpu.roll(tap(2, 0, m), m - 1, 0), 0.0)
        sides = low + high
        for start in (0, per_set):
            stop = start + per_set
            prod[a, s, start:stop] = sides[start:stop] + tap(1, start, stop)

    def sends(s, k):
        return pltpu.make_async_remote_copy(
            src_ref=nbuf.at[s, k],
            dst_ref=rbuf.at[s, k],
            send_sem=n_send.at[s, k],
            recv_sem=n_recv.at[s, k],
            device_id={"tm": lax.rem(tm + 1, n_tm)},
            device_id_type=MESH,
        )

    def send(s, k):
        @pl.when(tm < n_tm - 1)
        def _():
            sends(s, k).start()

    def wait_weights(a):
        for c in range(3):
            w_copies[a][c].wait()

    def early(s):
        if s == 0:
            wait_weights(0)
            wait_weights(1)
        product(0, s)
        nbuf[s, 1] = prod[0, s, per_set:].astype(BF16)
        send(s, 1)
        product(1, s)
        nbuf[s, 0] = (prod[0, s, :per_set] + prod[1, s, per_set:]).astype(BF16)
        send(s, 0)

    early(0)

    @pl.when(hh > 0)
    def _():
        to_next.wait_recv()
        for f in range(frames):
            place(-1, f, activate(top_vm[f]))

    @pl.when(hh == 0)
    def _():
        for f in range(frames):
            place(-1, f, jnp.zeros((cols, channels), BF16))

    @pl.when(hh < n_h - 1)
    def _():
        to_last.wait_recv()
        for f in range(frames):
            place(rows, f, activate(bot_vm[f]))

    @pl.when(hh == n_h - 1)
    def _():
        for f in range(frames):
            place(rows, f, jnp.zeros((cols, channels), BF16))

    wait_weights(2)
    early(1)
    product(2, 0)
    product(2, 1)

    bias = bias_ref[...]
    for s in range(2):
        for k in (1, 0):

            @pl.when(tm > 0)
            def _():
                sends(s, k).wait_recv()

            own = prod[2, s, k * per_set : (k + 1) * per_set]
            first = prod[0, s, :per_set]
            other = prod[1, s, :per_set]
            if k == 1:
                own = own + other
            else:
                first = first + other
            earlier = jnp.where(tm == 0, first, rbuf[s, k].astype(F32))
            value = (own + earlier + bias).astype(BF16)
            for q, i in enumerate(row_sets[s]):
                out_ref[k, i] = value[q * cols : (q + 1) * cols]

    for copy in shares:
        copy.wait_send()

    @pl.when(hh < n_h - 1)
    def _():
        to_next.wait_send()

    @pl.when(hh > 0)
    def _():
        to_last.wait_send()

    @pl.when(tm < n_tm - 1)
    def _():
        for s in range(2):
            for k in range(2):
                sends(s, k).wait_send()


def solution(mesh):
    n_tm, n_h = mesh.shape["tm"], mesh.shape["height"]

    def on_device(features, gain, shift, kernel, bias):
        frames, rows, cols, channels = features.shape
        c_out = kernel.shape[-1]
        assert frames == 2 and rows == 4
        per_set = 2 * cols
        vmem = pl.BlockSpec(memory_space=pltpu.VMEM)
        hbm = pl.BlockSpec(memory_space=pltpu.HBM)
        dma = pltpu.SemaphoreType.DMA
        return pl.pallas_call(
            functools.partial(body, n_tm, n_h),
            out_shape=pltpu.VMEM((frames, rows, cols, c_out), BF16),
            in_specs=[hbm] * 5,
            out_specs=vmem,
            scratch_shapes=[
                pltpu.VMEM((frames, rows, cols, channels), BF16),
                pltpu.VMEM((1, channels), F32),
                pltpu.VMEM((1, channels), F32),
                pltpu.VMEM((1, c_out), F32),
                pltpu.VMEM((3, 3, 3, channels, c_out), BF16),
                pltpu.VMEM((frames, cols, channels), BF16),
                pltpu.VMEM((frames, cols, channels), BF16),
                pltpu.VMEM((n_tm * n_h, 1, LANES), F32),
                pltpu.VMEM((2, frames * per_set, 3 * channels), BF16),
                pltpu.VMEM((3, 2, frames * per_set, c_out), F32),
                pltpu.VMEM((2, 2, per_set, c_out), BF16),
                pltpu.VMEM((2, 2, per_set, c_out), BF16),
                dma((frames,)),
                dma((3,)),
                dma((3, 3)),
                dma((n_tm * n_h,)),
                dma((n_tm * n_h,)),
                dma((2,)),
                dma((2,)),
                dma((2, 2)),
                dma((2, 2)),
            ],
            compiler_params=pltpu.CompilerParams(
                collective_id=0, has_side_effects=True, vmem_limit_bytes=67_043_328 - 640 * 2**10
            ),
        )(features, gain.reshape(1, -1), shift.reshape(1, -1), kernel, bias.reshape(1, -1))

    placed = (P(("clips", "tm"), "height", None, None), P(), P(), P(), P())
    return jax.shard_map(
        on_device,
        mesh=mesh,
        in_specs=placed,
        out_specs=P(("clips", "tm"), "height", None, None),
        check_vma=False,
    )
```
